32 devices in a mesh: groups: 2 (over y), section: 4 (over z), seq: 4 (over x, core).
Axes of the slice: x: 2, y: 2, z: 4, core: 2. Of those that a mesh axis runs over, the one named last changes fastest.
Arguments:
- tokens: bfloat16 [8, 256, 1440], P('groups', 'seq'), parts along dimension 0, may hold values from -6 to 6
- block_order: int32 [8], P('groups'), parts along dimension 0, may hold values from 0 to 3, each once
- prompt_lengths: int32 [8], P('groups'), parts along dimension 0, may hold values from 1 to 256, 576 in all
- norm_gain: float32 [4, 1440], P('section'), may hold values from 0.1 to 1.9
- w_query: bfloat16 [4, 1440, 2048], P('section', None, 'seq'), may hold values from -4 to 4
- w_key_value: bfloat16 [4, 1440, 512], P('section'), may hold values from -4 to 4
- w_out: bfloat16 [4, 2048, 1440], P('section', 'seq'), may hold values from -0.125 to 0.125
- sink_logits: float32 [4, 32], P('section'), may hold values from 0 to 4
Outputs:
- hidden_states: bfloat16 [4, 8, 256, 1440], P('section', 'groups', 'seq'), parts along dimension 1
- layer_cache: bfloat16 [4, 8, 256, 512], P('section', 'groups', 'seq'), parts along dimension 1
The draws below stay inside these ranges and needn't reach their ends.
There are 2 independent parts, one for each index of `groups`. The reference program is written for one: setup_inputs(seed, part) draws one part's arguments, and reference() takes and returns one part's arrays. A program takes and returns all parts, laid end to end along the dimension named above; an argument that names none is the same for every part. Nothing has to cross between parts.
Inputs may be any that keep to these rules, and one draw needn't show every extreme that they name: `block_order`: each of 0 to 3 exactly once. `prompt_lengths`: the longest prompt is full.
All inputs are finite; a program needn't handle non-finite values.
Results may differ from the reference program's by a relative error of at most 0.024.
Values may be sent and summed in bfloat16 or wider, within the bound.
A program may use at most 128 MiB of HBM per device.

```python
import math
import jax
import jax.numpy as jnp
import numpy as np
from jax import lax

D = 1440
HEADS = 32
KV_HEADS = 4
HEAD_DIM = 64
WIN = 128
MICRO = 4
BLOCK = 256
LAYERS = 4


def base_keys(key):
    drawn = jax.random.normal(jax.random.fold_in(key, 7), (LAYERS, D, 2 * KV_HEADS * HEAD_DIM), jnp.float32)
    return drawn * D ** (-0.5)


def draw_w_key_value(key, part):
    return jnp.clip(base_keys(key), -4.0, 4.0).astype(jnp.bfloat16)


def draw_w_query(key, part):
    drawn = jax.random.normal(jax.random.fold_in(key, 1), (LAYERS, D, HEADS * HEAD_DIM), jnp.float32) * D ** (-0.5)
    return jnp.clip(drawn, -4.0, 4.0).astype(jnp.bfloat16)


def steps_of(own_key, extent, cuts, least, top_value):
    def one(position, blocks):
        heights = jax.random.uniform(jax.random.fold_in(jax.random.fold_in(own_key, 6), position), (blocks,), jnp.float32, least / len(cuts), top_value / len(cuts))
        return jnp.repeat(jnp.exp(heights), extent[position] // blocks).reshape((-1,) + (1,) * (len(extent) - position - 1))

    loudness = one(*cuts[0])
    for cut in cuts[1:]:
        loudness = loudness * one(*cut)
    return loudness


def length_profile(count, total, limit, lean):
    loads = [(1 << 20) // math.isqrt(rank ** lean) + 1 for rank in range(2, count + 1)]
    surplus, holding = total - limit - (count - 1), [1] * (count - 1)
    while surplus > 0:
        free = [i for i in range(count - 1) if holding[i] < limit]
        whole, left = sum([loads[i] for i in free]), surplus
        for i in free:
            addition = min(limit - holding[i], max(1, left * loads[i] // whole), surplus)
            holding[i] = holding[i] + addition
            surplus = surplus - addition
    return np.array([limit] + holding)


def uneven_parts(key, amount, total, most, lean):
    if amount == 2:
        one = jax.random.randint(key, (), max(1, total - most), min(most, total - 1) + 1)
        return jnp.stack([one, total - one])
    tallies = jnp.asarray(length_profile(amount, total, most, lean), jnp.int32)
    couples = (amount - 1) // 2
    giver, receiver = tallies[1:1 + 2 * couples:2], tallies[2:2 + 2 * couples:2]
    margin = jnp.minimum(giver - 1, most - receiver)
    shifted = jax.random.randint(jax.random.fold_in(key, 1), (couples,), 0, 1 << 20) % (margin + 1)
    tallies = tallies.at[1:1 + 2 * couples:2].set(giver - shifted).at[2:2 + 2 * couples:2].set(receiver + shifted)
    return tallies[jax.random.permutation(jax.random.fold_in(key, 2), amount)]


def noise(rng, shape, spread, reach, pieces=(), kind=jnp.bfloat16):
    level = steps_of(rng, shape, pieces, -0.22, 0.18) if pieces else 1.0
    entries = jax.random.normal(rng, shape, jnp.float32) * spread * level
    return jnp.minimum(jnp.maximum(entries, -reach), reach).astype(kind)


def setup_inputs(seed: int = 0, part: int = 0) -> dict:
    arg_keys = jax.random.split(jax.random.key(seed), 9)
    part_keys = jax.random.split(jax.random.fold_in(arg_keys[8], part), 9)
    tokens = noise(part_keys[0], (MICRO, BLOCK, D), 1.0, 6.0, ((1, 4),))
    block_order = jax.random.permutation(part_keys[1], MICRO).astype(jnp.int32)
    prompt_lengths = uneven_parts(part_keys[2], MICRO, 9 * MICRO * BLOCK // 16, BLOCK, 2).astype(jnp.int32)
    norm_gain = jnp.clip(1.0 + 0.18 * jax.random.normal(arg_keys[3], (LAYERS, D), jnp.float32), 0.1, 1.9)
    w_query = draw_w_query(jax.random.fold_in(arg_keys[8], 71), part)
    w_key_value = draw_w_key_value(jax.random.fold_in(arg_keys[8], 71), part)
    w_out = noise(arg_keys[6], (LAYERS, HEADS * HEAD_DIM, D), (HEADS * HEAD_DIM) ** -0.5, 0.125, ((0, 4), (1, 4)))
    sink_logits = jnp.clip(4.0 * jax.random.uniform(arg_keys[7], (LAYERS, HEADS), jnp.float32) ** steps_of(arg_keys[7], (LAYERS, HEADS), ((0, 4),), -0.2, 0.2), 0.0, 4.0)
    return dict(tokens=tokens, block_order=block_order, prompt_lengths=prompt_lengths, norm_gain=norm_gain, w_query=w_query, w_key_value=w_key_value, w_out=w_out, sink_logits=sink_logits)


THETA = 150000.0
EPSILON = 1e-05

def rotary(positions, head_size):
    half = head_size // 2
    freq = jnp.exp(jnp.arange(half, dtype=jnp.float32) * (-2.0 * math.log(THETA) / head_size))
    angles = positions.astype(jnp.float32)[:, None] * freq[None, :]
    return (jnp.cos(angles)[:, None, :], jnp.sin(angles)[:, None, :])

def rotate(values, cosine, sine):
    half = values.shape[-1] // 2
    first = values[..., :half]
    second = values[..., half:]
    return jnp.concatenate([first * cosine - second * sine, second * cosine + first * sine], -1)

def layer_step(hidden, gain, w_query, w_key_value, w_out, sinks, cosine, sine, allowed):
    group = HEADS // KV_HEADS
    kv_width = KV_HEADS * HEAD_DIM
    count = hidden.shape[0]
    widened = hidden.astype(jnp.float32)
    scale = lax.rsqrt(lax.optimization_barrier(jnp.mean(widened * widened, -1, keepdims=True)) + EPSILON)
    normed = (widened * scale * gain).astype(jnp.bfloat16)
    queries = jnp.dot(normed, w_query, preferred_element_type=jnp.float32).reshape(count, HEADS, HEAD_DIM)
    queries = rotate(queries, cosine, sine).astype(jnp.bfloat16)
    projected = jnp.dot(normed, w_key_value, preferred_element_type=jnp.float32)
    keys = rotate(projected[:, :kv_width].reshape(count, KV_HEADS, HEAD_DIM), cosine, sine).reshape(count, kv_width)
    cache = jnp.concatenate([keys, projected[:, kv_width:]], 1).astype(jnp.bfloat16)
    key_heads = cache[:, :kv_width].reshape(count, KV_HEADS, HEAD_DIM).astype(jnp.float32)
    value_heads = cache[:, kv_width:].reshape(count, KV_HEADS, HEAD_DIM).astype(jnp.float32)
    grouped = queries.reshape(count, KV_HEADS, group, HEAD_DIM).astype(jnp.float32)
    scores = jnp.einsum('qkgd,skd->kgqs', grouped, key_heads) * 0.125
    sink = sinks.reshape(KV_HEADS, group)[:, :, None]
    masked = jnp.where(allowed, scores, jnp.float32(-1e+30))
    top = jnp.maximum(lax.optimization_barrier(jnp.max(masked, -1)), sink)
    expo = jnp.where(allowed, jnp.exp(scores - top[..., None]), jnp.float32(0.0))
    total = lax.optimization_barrier(jnp.sum(expo, -1)) + jnp.exp(sink - top)
    weights = (expo / total[..., None]).astype(jnp.bfloat16)
    context = jnp.einsum('kgqs,skd->qkgd', weights.astype(jnp.float32), value_heads)
    context = context.reshape(count, HEADS * HEAD_DIM).astype(jnp.bfloat16)
    output = jnp.dot(context, w_out, preferred_element_type=jnp.float32)
    return ((widened + output).astype(jnp.bfloat16), cache)

def reference(tokens, block_order, prompt_lengths, norm_gain, w_query, w_key_value, w_out, sink_logits):
    positions = jnp.arange(BLOCK, dtype=jnp.int32)
    cosine, sine = rotary(positions, HEAD_DIM)
    within = (positions[None, :] <= positions[:, None]) & (positions[:, None] - positions[None, :] < WIN)
    hidden_rows = [[] for layer in range(LAYERS)]
    cache_rows = [[] for layer in range(LAYERS)]
    for slot in range(MICRO):
        block = block_order[slot]
        hidden = lax.dynamic_index_in_dim(tokens, block, 0, keepdims=False)
        length = lax.dynamic_index_in_dim(prompt_lengths, block, 0, keepdims=False)
        allowed = within & ((positions[None, :] < length) | (positions[None, :] == positions[:, None]))
        for layer in range(LAYERS):
            hidden, cache = layer_step(hidden, norm_gain[layer], w_query[layer], w_key_value[layer], w_out[layer], sink_logits[layer], cosine, sine, allowed)
            hidden_rows[layer].append(hidden)
            cache_rows[layer].append(cache)
    hidden_states = jnp.stack([jnp.stack(row) for row in hidden_rows])
    layer_cache = jnp.stack([jnp.stack(row) for row in cache_rows])
    return (hidden_states, layer_cache)
```

```python
import functools
import math

import jax
import jax.numpy as jnp
from jax import lax
from jax.experimental import pallas as pl
from jax.experimental.pallas import tpu as pltpu
from jax.sharding import PartitionSpec as P

HEAD_DIM = 64
WIN = 128
LANES = 128


THETA = 150000.0
EPSILON = 1e-05
MESH = pl.DeviceIdType.MESH
F32 = jnp.float32
BF16 = jnp.bfloat16
QUERY_CUTS = 3
OUT_CUTS = 4


def rotary(positions, head_size):
    half = head_size // 2
    freq = jnp.exp(jnp.arange(half, dtype=F32) * (-2.0 * math.log(THETA) / head_size))
    angles = positions.astype(F32)[:, None] * freq[None, :]
    return jnp.cos(angles), jnp.sin(angles)


def kernel(
    shape,
    order_ref, length_ref, sink_ref,
    tokens_ref, gain_ref, cos_ref, sin_ref, pair_ref, query_hbm, out_hbm,
    hidden_ref, cache_ref,
    query_w, out_w, arrive, window, hbuf, normed_ref, qbuf, cbuf,
    local_sem, x_send, x_recv, y_send, y_recv, d_send, d_recv, own_send, own_recv,
    w_send, w_recv, z_send, z_recv,
):
    groups, sections, seq = shape
    chips = seq // 2
    g = lax.axis_index("groups")
    sec = lax.axis_index("section")
    q = lax.axis_index("seq")
    chip, core = q // 2, q % 2
    partner = chip * 2 + (1 - core)
    micro, rows, width = tokens_ref.shape
    shard = query_w.shape[2]
    heads_width = seq * shard
    kv_width = pair_ref.shape[1] // 2
    kv_heads = kv_width // HEAD_DIM
    group = heads_width // kv_width
    keep = min(WIN, rows)
    depth = WIN // keep

    mine = [
        pltpu.make_async_copy(query_hbm, query_w.at[q], local_sem.at[0]),
        pltpu.make_async_copy(
            out_hbm, out_w.at[pl.ds(pl.multiple_of(q * shard, shard), shard)], local_sem.at[1]
        ),
    ]
    for copy in mine:
        copy.start()

    barrier = pltpu.get_barrier_semaphore()
    greeted = 0
    for d in range(1, seq):
        pl.semaphore_signal(barrier, 1, device_id={"seq": (q + d) % seq}, device_id_type=MESH)
        greeted += 1
    for e in range(1, groups):
        pl.semaphore_signal(barrier, 1, device_id={"groups": (g + e) % groups}, device_id_type=MESH)
        greeted += 1
    for s in sorted({1 % sections, (sections - 1) % sections} - {0}):
        pl.semaphore_signal(barrier, 1, device_id={"section": (sec + s) % sections}, device_id_type=MESH)
        greeted += 1
    for off in range(1, depth + 1):

        @pl.when(q < off)
        def _():
            window[:, off - 1] = jnp.zeros((micro, keep, 2 * kv_width), BF16)

    pl.semaphore_wait(barrier, greeted)

    cuts = (QUERY_CUTS, OUT_CUTS)
    lengths = (width // groups // QUERY_CUTS, shard // groups // OUT_CUTS)

    def piece(kind, owner, part, k):
        size = lengths[kind]
        first = (part * cuts[kind] + k) * size
        if kind == 0:
            return query_w.at[owner, pl.ds(pl.multiple_of(first, 16), size)]
        return out_w.at[pl.ds(pl.multiple_of(owner * shard + first, 16), size)]

    def whole(kind, owner):
        if kind == 0:
            return query_w.at[owner]
        return out_w.at[pl.ds(pl.multiple_of(owner * shard, shard), shard)]

    def remote(ref, send, recv, target):
        return pltpu.make_async_remote_copy(
            src_ref=ref, dst_ref=ref, send_sem=send, recv_sem=recv,
            device_id=target, device_id_type=MESH,
        )

    def x_copy(kind, d, k, owner):
        return remote(
            piece(kind, owner, g, k), x_send.at[kind, d, k], x_recv.at[kind, d, k],
            {"seq": ((chip + d) % chips) * 2 + core},
        )

    def y_copy(kind, d, k, e, owner, part):
        return remote(
            piece(kind, owner, part, k), y_send.at[kind, d, k, e], y_recv.at[kind, d, k, e],
            {"groups": (g + e) % groups},
        )

    def d_copy(kind, d, k, e, owner):
        return remote(
            piece(kind, owner, (g - e + groups) % groups, k), d_send.at[kind, d, k, e],
            d_recv.at[kind, d, k, e], {"seq": partner},
        )

    def own_copy(kind, owner):
        return remote(whole(kind, owner), own_send.at[kind], own_recv.at[kind], {"seq": partner})

    plan = [(kind, k, d) for kind in range(2) for k in range(cuts[kind]) for d in range(1, chips)]
    for kind in range(2):
        mine[kind].wait()
        for k in range(cuts[kind]):
            for d in range(1, chips):
                x_copy(kind, d, k, q).start()
        own_copy(kind, q).start()

    def source(d, which):
        return ((chip - d + chips) % chips) * 2 + which

    def relay_y(kind, k, d):
        for e in range(1, groups):
            y_copy(kind, d, k, e, source(d, core), (g - e + groups) % groups).wait_recv()
            d_copy(kind, d, k, e, source(d, core)).start()

    previous = None
    for kind, k, d in plan:
        x_copy(kind, d, k, source(d, core)).wait_recv()
        for e in range(1, groups):
            y_copy(kind, d, k, e, source(d, core), g).start()
        d_copy(kind, d, k, 0, source(d, core)).start()
        if previous is not None:
            relay_y(*previous)
        previous = (kind, k, d)
    if previous is not None:
        relay_y(*previous)
    for kind in range(2):
        own_copy(kind, partner).wait_recv()
    for kind, k, d in plan:
        for e in range(groups):
            d_copy(kind, d, k, e, source(d, 1 - core)).wait_recv()

    lane = lax.broadcasted_iota(jnp.int32, (rows, LANES), 1)
    first_half = (lane % HEAD_DIM) < (HEAD_DIM // 2)
    low = lane < HEAD_DIM
    cosine = cos_ref[...]
    sine = sin_ref[...]
    half = HEAD_DIM // 2

    def rotate(tile):
        swapped = jnp.where(
            first_half, pltpu.roll(tile, LANES - half, 1), pltpu.roll(tile, half, 1)
        )
        return tile * cosine + swapped * sine

    def z_copy(t):
        return pltpu.make_async_remote_copy(
            src_ref=hidden_ref.at[t], dst_ref=arrive.at[t], send_sem=z_send.at[t],
            recv_sem=z_recv.at[t], device_id={"section": (sec + 1) % sections}, device_id_type=MESH,
        )

    def w_copy(t, off):
        return pltpu.make_async_remote_copy(
            src_ref=cache_ref.at[t, pl.ds(rows - keep, keep)], dst_ref=window.at[t, off - 1],
            send_sem=w_send.at[t, off - 1], recv_sem=w_recv.at[t, off - 1],
            device_id={"seq": (q + off) % seq}, device_id_type=MESH,
        )

    def slot(t, carry):
        block = order_ref[t]
        length = length_ref[block]

        @pl.when(sec == 0)
        def _():
            hbuf[...] = tokens_ref[block]

        @pl.when(sec > 0)
        def _():
            z_copy(t).wait_recv()
            hbuf[...] = arrive[t]

        widened = hbuf[...].astype(F32)
        scale = lax.rsqrt(jnp.mean(widened * widened, -1, keepdims=True) + EPSILON)
        normed_ref[...] = (widened * scale * gain_ref[...]).astype(BF16)
        normed = normed_ref[...]
        projected = jnp.dot(normed, pair_ref[...], preferred_element_type=F32)
        for p in range(kv_width // LANES):
            tile = slice(p * LANES, (p + 1) * LANES)
            cache_ref[t, :, tile] = rotate(projected[:, tile]).astype(BF16)
        cache_ref[t, :, kv_width:] = projected[:, kv_width:].astype(BF16)
        for off in range(1, depth + 1):

            @pl.when(q + off < seq)
            def _():
                w_copy(t, off).start()

        for s in range(seq):
            queries = jnp.dot(normed, query_w[s], preferred_element_type=F32)
            for p in range(shard // LANES):
                rotated = rotate(queries[:, p * LANES:(p + 1) * LANES]) * 0.125
                qbuf[:, s * shard + p * LANES:s * shard + (p + 1) * LANES] = rotated.astype(BF16)

        for off in range(1, depth + 1):

            @pl.when(q >= off)
            def _():
                w_copy(t, off).wait_recv()

        span = WIN + rows
        row = lax.broadcasted_iota(jnp.int32, (rows, span), 0)
        col = lax.broadcasted_iota(jnp.int32, (rows, span), 1) - WIN
        column = col + q * rows
        allowed = (col <= row) & (row - col < WIN) & (column >= 0)
        allowed = allowed & ((column < length) | (col == row))
        bias = jnp.where(allowed, F32(0.0), F32(-1e30))
        tiles = group // 2
        for h in range(kv_heads):
            def span_of(first):
                at = slice(first, first + HEAD_DIM)
                parts = [window[t, off - 1, :, at] for off in range(depth, 0, -1)]
                head = jnp.concatenate(parts + [cache_ref[t, :, at]], 0)
                return jnp.concatenate([head, head], 1)

            keys = span_of(h * HEAD_DIM)
            values = span_of(kv_width + h * HEAD_DIM)
            stack, sinks = [], []
            for p in range(tiles):
                at = (h * tiles + p) * LANES
                pair = qbuf[:, at:at + LANES]
                zero = jnp.zeros_like(pair)
                stack += [jnp.where(low, pair, zero), jnp.where(low, zero, pair)]
                for j in range(2):
                    sinks.append(jnp.full((1, rows, 1), sink_ref[h * group + 2 * p + j], F32))
            sink = jnp.concatenate(sinks, 0)
            scores = lax.dot_general(
                jnp.concatenate(stack, 0), keys, (((1,), (1,)), ((), ())),
                preferred_element_type=F32,
            ).reshape(group, rows, span)
            masked = jnp.where(bias[None] < 0, F32(-1e30), scores)
            top = jnp.maximum(jnp.max(masked, -1, keepdims=True), sink)
            expo = jnp.exp(masked - top)
            total = jnp.sum(expo, -1, keepdims=True) + jnp.exp(sink - top)
            weights = (expo * (1.0 / total)).astype(BF16).reshape(group * rows, span)
            context = jnp.dot(weights, values, preferred_element_type=F32)
            for p in range(tiles):
                at = (h * tiles + p) * LANES
                one = context[2 * p * rows:(2 * p + 1) * rows]
                two = context[(2 * p + 1) * rows:(2 * p + 2) * rows]
                cbuf[:, at:at + LANES] = jnp.where(low, one, two).astype(BF16)
        output = jnp.dot(cbuf[...], out_w[...], preferred_element_type=F32)
        hidden_ref[t] = (hbuf[...].astype(F32) + output).astype(BF16)

        @pl.when(sec + 1 < sections)
        def _():
            z_copy(t).start()

        return carry

    lax.fori_loop(0, micro, slot, 0)

    for kind, k, d in plan:
        x_copy(kind, d, k, q).wait_send()
        for e in range(1, groups):
            y_copy(kind, d, k, e, source(d, core), g).wait_send()
        for e in range(groups):
            d_copy(kind, d, k, e, source(d, core)).wait_send()
    for kind in range(2):
        own_copy(kind, q).wait_send()
    for t in range(micro):
        for off in range(1, depth + 1):

            @pl.when(q + off < seq)
            def _():
                w_copy(t, off).wait_send()

        @pl.when(sec + 1 < sections)
        def _():
            z_copy(t).wait_send()


def per_device(
    shape,
    tokens, block_order, prompt_lengths, norm_gain, w_query, w_key_value, w_out, sink_logits
):
    groups, sections, seq = shape
    micro, rows, width = tokens.shape
    shard = w_query.shape[2]
    pair_width = w_key_value.shape[2]
    chips = seq // 2
    keep = min(WIN, rows)
    depth = WIN // keep
    positions = lax.axis_index("seq") * rows + jnp.arange(rows, dtype=jnp.int32)
    cosine, sine = rotary(positions, HEAD_DIM)
    repeat = LANES // HEAD_DIM
    cosine = jnp.tile(jnp.concatenate([cosine, cosine], 1), (1, repeat))
    sine = jnp.tile(jnp.concatenate([-sine, sine], 1), (1, repeat))
    most = max(QUERY_CUTS, OUT_CUTS)
    dma = pltpu.SemaphoreType.DMA
    vmem = pl.BlockSpec(memory_space=pltpu.VMEM)
    smem = pl.BlockSpec(memory_space=pltpu.SMEM)
    hbm = pl.BlockSpec(memory_space=pl.ANY)
    hidden, cache = pl.pallas_call(
        functools.partial(kernel, shape),
        out_shape=(
            jax.ShapeDtypeStruct((micro, rows, width), BF16),
            jax.ShapeDtypeStruct((micro, rows, pair_width), BF16),
        ),
        in_specs=[smem] * 3 + [vmem] * 5 + [hbm] * 2,
        out_specs=(vmem, vmem),
        scratch_shapes=[
            pltpu.VMEM((seq, width, shard), BF16),
            pltpu.VMEM((seq * shard, width), BF16),
            pltpu.VMEM((micro, rows, width), BF16),
            pltpu.VMEM((micro, depth, keep, pair_width), BF16),
            pltpu.VMEM((rows, width), BF16),
            pltpu.VMEM((rows, width), BF16),
            pltpu.VMEM((rows, seq * shard), BF16),
            pltpu.VMEM((rows, seq * shard), BF16),
            dma((2,)),
            dma((2, chips, most)),
            dma((2, chips, most)),
            dma((2, chips, most, groups)),
            dma((2, chips, most, groups)),
            dma((2, chips, most, groups)),
            dma((2, chips, most, groups)),
            dma((2,)),
            dma((2,)),
            dma((micro, depth)),
            dma((micro, depth)),
            dma((micro,)),
            dma((micro,)),
        ],
        compiler_params=pltpu.CompilerParams(
            collective_id=0, has_side_effects=True, vmem_limit_bytes=50 * 1024 * 1024
        ),
    )(
        block_order, prompt_lengths, sink_logits[0],
        tokens, norm_gain, cosine, sine, w_key_value[0], w_query[0], w_out[0],
    )
    return hidden[None], cache[None]


def solution(mesh):
    in_specs = (
        P("groups", "seq", None),
        P("groups"),
        P("groups"),
        P("section", None),
        P("section", None, "seq"),
        P("section", None, None),
        P("section", "seq", None),
        P("section", None),
    )
    out_specs = (P("section", "groups", "seq", None), P("section", "groups", "seq", None))
    shape = tuple(mesh.shape[name] for name in ("groups", "section", "seq"))
    return jax.shard_map(
        functools.partial(per_device, shape),
        mesh=mesh, in_specs=in_specs, out_specs=out_specs, check_vma=False,
    )
```

```python
import functools
import math

import jax
import jax.numpy as jnp
from jax import lax
from jax.experimental import pallas as pl
from jax.experimental.pallas import tpu as pltpu
from jax.sharding import PartitionSpec as P

HEAD_DIM = 64
WIN = 128
LANES = 128


THETA = 150000.0
EPSILON = 1e-05
MESH = pl.DeviceIdType.MESH
F32 = jnp.float32
BF16 = jnp.bfloat16
QUERY_CUTS = 3
OUT_CUTS = 3
HOP_CUTS = 3
EARLY = 4


def rotary(positions, head_size):
    half = head_size // 2
    freq = jnp.exp(jnp.arange(half, dtype=F32) * (-2.0 * math.log(THETA) / head_size))
    angles = positions.astype(F32)[:, None] * freq[None, :]
    return jnp.cos(angles), jnp.sin(angles)


def kernel(
    shape,
    order_ref, length_ref, sink_ref,
    tokens_ref, gain_ref, cos_ref, sin_ref, pair_ref, query_hbm, out_hbm,
    hidden_ref, cache_ref,
    query_w, out_w, arrive, window, hbuf, normed_ref, qbuf, cbuf,
    local_sem, x_send, x_recv, y_send, y_recv, d_send, d_recv, own_send, own_recv,
    w_send, w_recv, z_send, z_recv,
):
    groups, sections, seq = shape
    chips = seq // 2
    g = lax.axis_index("groups")
    sec = lax.axis_index("section")
    q = lax.axis_index("seq")
    chip, core = q // 2, q % 2
    partner = chip * 2 + (1 - core)
    micro, rows, width = tokens_ref.shape
    shard = query_w.shape[2]
    heads_width = seq * shard
    kv_width = pair_ref.shape[1] // 2
    kv_heads = kv_width // HEAD_DIM
    group = heads_width // kv_width
    keep = min(WIN, rows)
    depth = WIN // keep

    mine = [
        pltpu.make_async_copy(query_hbm, query_w.at[q], local_sem.at[0]),
        pltpu.make_async_copy(
            out_hbm, out_w.at[:, pl.ds(pl.multiple_of(q * shard, shard), shard)], local_sem.at[1]
        ),
    ]
    for copy in mine:
        copy.start()

    barrier = pltpu.get_barrier_semaphore()
    greeted = 0
    for d in range(1, seq):
        pl.semaphore_signal(barrier, 1, device_id={"seq": (q + d) % seq}, device_id_type=MESH)
        greeted += 1
    for e in range(1, groups):
        pl.semaphore_signal(barrier, 1, device_id={"groups": (g + e) % groups}, device_id_type=MESH)
        greeted += 1
    for s in sorted({1 % sections, (sections - 1) % sections} - {0}):
        pl.semaphore_signal(barrier, 1, device_id={"section": (sec + s) % sections}, device_id_type=MESH)
        greeted += 1
    for off in range(1, depth + 1):

        @pl.when(q < off)
        def _():
            window[:, off - 1] = jnp.zeros((micro, keep, 2 * kv_width), BF16)

    pl.semaphore_wait(barrier, greeted)

    cuts = (QUERY_CUTS, OUT_CUTS)
    lengths = (width // groups // QUERY_CUTS, width // groups // OUT_CUTS)

    def piece(kind, owner, part, k):
        size = lengths[kind]
        first = (part * cuts[kind] + k) * size
        if kind == 0:
            return query_w.at[owner, pl.ds(pl.multiple_of(first, 16), size)]
        return out_w.at[
            pl.ds(pl.multiple_of(first, 16), size), pl.ds(pl.multiple_of(owner * shard, shard), shard)
        ]

    def whole(kind, owner):
        if kind == 0:
            return query_w.at[owner]
        return out_w.at[:, pl.ds(pl.multiple_of(owner * shard, shard), shard)]

    def remote(ref, send, recv, target):
        return pltpu.make_async_remote_copy(
            src_ref=ref, dst_ref=ref, send_sem=send, recv_sem=recv,
            device_id=target, device_id_type=MESH,
        )

    def x_copy(kind, d, k, owner):
        return remote(
            piece(kind, owner, g, k), x_send.at[kind, d, k], x_recv.at[kind, d, k],
            {"seq": ((chip + d) % chips) * 2 + core},
        )

    def y_copy(kind, d, k, e, owner, part):
        return remote(
            piece(kind, owner, part, k), y_send.at[kind, d, k, e], y_recv.at[kind, d, k, e],
            {"groups": (g + e) % groups},
        )

    def d_copy(kind, d, k, e, owner):
        return remote(
            piece(kind, owner, (g - e + groups) % groups, k), d_send.at[kind, d, k, e],
            d_recv.at[kind, d, k, e], {"seq": partner},
        )

    def own_copy(kind, owner):
        return remote(whole(kind, owner), own_send.at[kind], own_recv.at[kind], {"seq": partner})

    plan = [(kind, k, d) for kind in range(2) for k in range(cuts[kind]) for d in range(1, chips)]
    for kind in range(2):
        mine[kind].wait()
        for k in range(cuts[kind]):
            for d in range(1, chips):
                x_copy(kind, d, k, q).start()
        own_copy(kind, q).start()

    lane = lax.broadcasted_iota(jnp.int32, (rows, LANES), 1)
    first_half = (lane % HEAD_DIM) < (HEAD_DIM // 2)
    low = lane < HEAD_DIM
    cosine = cos_ref[...]
    sine = sin_ref[...]
    half = HEAD_DIM // 2

    def rotate(tile):
        swapped = jnp.where(
            first_half, pltpu.roll(tile, LANES - half, 1), pltpu.roll(tile, half, 1)
        )
        return tile * cosine + swapped * sine

    step = -(-width // (HOP_CUTS * LANES)) * LANES
    edges = [(c * step, min(step, width - c * step)) for c in range(HOP_CUTS)]

    def z_copy(t, c):
        columns = pl.ds(*edges[c])
        return pltpu.make_async_remote_copy(
            src_ref=hidden_ref.at[t, :, columns], dst_ref=arrive.at[t, :, columns],
            send_sem=z_send.at[t, c], recv_sem=z_recv.at[t, c], device_id={"section": (sec + 1) % sections}, device_id_type=MESH,
        )

    def w_copy(t, off, side):
        columns = pl.ds(side * kv_width, kv_width)
        return pltpu.make_async_remote_copy(
            src_ref=cache_ref.at[t, pl.ds(rows - keep, keep), columns],
            dst_ref=window.at[t, off - 1, :, columns],
            send_sem=w_send.at[t, off - 1, side], recv_sem=w_recv.at[t, off - 1, side],
            device_id={"seq": (q + off) % seq}, device_id_type=MESH,
        )

    def enter(t):
        block = order_ref[t]

        @pl.when(sec == 0)
        def _():
            hbuf[t] = tokens_ref[block]

        @pl.when(sec > 0)
        def _():
            for c in range(HOP_CUTS):
                z_copy(t, c).wait_recv()
            hbuf[t] = arrive[t]

        widened = hbuf[t].astype(F32)
        scale = lax.rsqrt(jnp.mean(widened * widened, -1, keepdims=True) + EPSILON)
        normed_ref[t] = (widened * scale * gain_ref[...]).astype(BF16)
        keys = jnp.dot(normed_ref[t], pair_ref[:, :kv_width], preferred_element_type=F32)
        for p in range(kv_width // LANES):
            tile = slice(p * LANES, (p + 1) * LANES)
            cache_ref[t, :, tile] = rotate(keys[:, tile]).astype(BF16)
        for off in range(1, depth + 1):

            @pl.when(q + off < seq)
            def _():
                w_copy(t, off, 0).start()

        values = jnp.dot(normed_ref[t], pair_ref[:, kv_width:], preferred_element_type=F32)
        cache_ref[t, :, kv_width:] = values.astype(BF16)
        for off in range(1, depth + 1):

            @pl.when(q + off < seq)
            def _():
                w_copy(t, off, 1).start()

    @pl.when(sec == 0)
    def _():
        @pl.loop(0, micro)
        def _(t):
            enter(t)

    def source(d, which):
        return ((chip - d + chips) % chips) * 2 + which

    def relay_y(kind, k, d):
        for e in range(1, groups):
            y_copy(kind, d, k, e, source(d, core), (g - e + groups) % groups).wait_recv()
            d_copy(kind, d, k, e, source(d, core)).start()

    previous = None
    for kind, k, d in plan:
        x_copy(kind, d, k, source(d, core)).wait_recv()
        for e in range(1, groups):
            y_copy(kind, d, k, e, source(d, core), g).start()
        d_copy(kind, d, k, 0, source(d, core)).start()
        if previous is not None:
            relay_y(*previous)
        previous = (kind, k, d)
    if previous is not None:
        relay_y(*previous)
    for kind in range(2):
        own_copy(kind, partner).wait_recv()
    for kind, k, d in plan:
        for e in range(groups):
            d_copy(kind, d, k, e, source(d, 1 - core)).wait_recv()

    def slot(t, carry):
        @pl.when(sec > 0)
        def _():
            enter(t)

        length = length_ref[order_ref[t]]
        normed = normed_ref[t]

        def ask(s):
            queries = jnp.dot(normed, query_w[s], preferred_element_type=F32)
            for p in range(shard // LANES):
                rotated = rotate(queries[:, p * LANES:(p + 1) * LANES]) * 0.125
                qbuf[:, s * shard + p * LANES:s * shard + (p + 1) * LANES] = rotated.astype(BF16)

        per_head = seq // kv_heads
        early = min(EARLY, kv_heads)
        for s in range(early * per_head):
            ask(s)

        for off in range(1, depth + 1):

            @pl.when(q >= off)
            def _():
                w_copy(t, off, 0).wait_recv()
                w_copy(t, off, 1).wait_recv()

        span = WIN + rows
        row = lax.broadcasted_iota(jnp.int32, (rows, span), 0)
        col = lax.broadcasted_iota(jnp.int32, (rows, span), 1) - WIN
        column = col + q * rows
        allowed = (col <= row) & (row - col < WIN) & (column >= 0)
        allowed = allowed & ((column < length) | (col == row))
        bias = jnp.where(allowed, F32(0.0), F32(-1e30))
        tiles = group // 2

        def span_of(first):
            at = slice(first, first + HEAD_DIM)
            parts = [window[t, off - 1, :, at] for off in range(depth, 0, -1)]
            return jnp.concatenate(parts + [cache_ref[t, :, at]], 0)

        def score(h):
            head = span_of(h * HEAD_DIM)
            stack = []
            for p in range(tiles):
                at = (h * tiles + p) * LANES
                pair = qbuf[:, at:at + LANES]
                zero = jnp.zeros_like(pair)
                stack += [jnp.where(low, pair, zero), jnp.where(low, zero, pair)]
            return lax.dot_general(
                jnp.concatenate(stack, 0), jnp.concatenate([head, head], 1),
                (((1,), (1,)), ((), ())), preferred_element_type=F32,
            )

        def mix(h, scores):
            head = span_of(kv_width + h * HEAD_DIM)
            values = jnp.concatenate([head, head, jnp.ones((span, LANES), BF16)], 1)
            expos, rest = [], []
            for j in range(group):
                sink = sink_ref[h * group + j]
                masked = scores[j * rows:(j + 1) * rows] + bias
                top = jnp.maximum(jnp.max(masked, -1, keepdims=True), sink)
                expos.append(jnp.exp(masked - top).astype(BF16))
                rest.append(jnp.exp(sink - top))
            summed = jnp.dot(jnp.concatenate(expos, 0), values, preferred_element_type=F32)
            for p in range(tiles):
                at = (h * tiles + p) * LANES
                sides = []
                for j in (2 * p, 2 * p + 1):
                    some = summed[j * rows:(j + 1) * rows]
                    sides.append((some[:, :LANES], some[:, LANES:] + rest[j]))
                context = jnp.where(low, sides[0][0], sides[1][0])
                context = context / jnp.where(low, sides[0][1], sides[1][1])
                cbuf[:, at:at + LANES] = context.astype(BF16)

        scores = score(0)
        for h in range(kv_heads):
            following = score(h + 1) if h + 1 < kv_heads else None
            if h + early < kv_heads:
                for s in range((h + early) * per_head, (h + early + 1) * per_head):
                    ask(s)
            mix(h, scores)
            scores = following
        for c, (first, size) in enumerate(edges):
            output = lax.dot_general(
                cbuf[...], out_w[first:first + size], (((1,), (1,)), ((), ())),
                preferred_element_type=F32,
            )
            columns = slice(first, first + size)
            hidden_ref[t, :, columns] = (hbuf[t, :, columns].astype(F32) + output).astype(BF16)

            @pl.when(sec + 1 < sections)
            def _():
                z_copy(t, c).start()

        return carry

    lax.fori_loop(0, micro, slot, 0)

    for kind, k, d in plan:
        x_copy(kind, d, k, q).wait_send()
        for e in range(1, groups):
            y_copy(kind, d, k, e, source(d, core), g).wait_send()
        for e in range(groups):
            d_copy(kind, d, k, e, source(d, core)).wait_send()
    for kind in range(2):
        own_copy(kind, q).wait_send()
    for t in range(micro):
        for off in range(1, depth + 1):

            @pl.when(q + off < seq)
            def _():
                w_copy(t, off, 0).wait_send()
                w_copy(t, off, 1).wait_send()

        @pl.when(sec + 1 < sections)
        def _():
            for c in range(HOP_CUTS):
                z_copy(t, c).wait_send()


def per_device(
    shape,
    tokens, block_order, prompt_lengths, norm_gain, w_query, w_key_value, w_out, sink_logits
):
    groups, sections, seq = shape
    micro, rows, width = tokens.shape
    shard = w_query.shape[2]
    pair_width = w_key_value.shape[2]
    chips = seq // 2
    keep = min(WIN, rows)
    depth = WIN // keep
    positions = lax.axis_index("seq") * rows + jnp.arange(rows, dtype=jnp.int32)
    cosine, sine = rotary(positions, HEAD_DIM)
    repeat = LANES // HEAD_DIM
    cosine = jnp.tile(jnp.concatenate([cosine, cosine], 1), (1, repeat))
    sine = jnp.tile(jnp.concatenate([-sine, sine], 1), (1, repeat))
    most = max(QUERY_CUTS, OUT_CUTS)
    dma = pltpu.SemaphoreType.DMA
    vmem = pl.BlockSpec(memory_space=pltpu.VMEM)
    smem = pl.BlockSpec(memory_space=pltpu.SMEM)
    hbm = pl.BlockSpec(memory_space=pl.ANY)
    hidden, cache = pl.pallas_call(
        functools.partial(kernel, shape),
        out_shape=(
            jax.ShapeDtypeStruct((micro, rows, width), BF16),
            jax.ShapeDtypeStruct((micro, rows, pair_width), BF16),
        ),
        in_specs=[smem] * 3 + [vmem] * 5 + [hbm] * 2,
        out_specs=(vmem, vmem),
        scratch_shapes=[
            pltpu.VMEM((seq, width, shard), BF16),
            pltpu.VMEM((width, seq * shard), BF16),
            pltpu.VMEM((micro, rows, width), BF16),
            pltpu.VMEM((micro, depth, keep, pair_width), BF16),
            pltpu.VMEM((micro, rows, width), BF16),
            pltpu.VMEM((micro, rows, width), BF16),
            pltpu.VMEM((rows, seq * shard), BF16),
            pltpu.VMEM((rows, seq * shard), BF16),
            dma((2,)),
            dma((2, chips, most)),
            dma((2, chips, most)),
            dma((2, chips, most, groups)),
            dma((2, chips, most, groups)),
            dma((2, chips, most, groups)),
            dma((2, chips, most, groups)),
            dma((2,)),
            dma((2,)),
            dma((micro, depth, 2)),
            dma((micro, depth, 2)),
            dma((micro, HOP_CUTS)),
            dma((micro, HOP_CUTS)),
        ],
        compiler_params=pltpu.CompilerParams(
            collective_id=0, has_side_effects=True, vmem_limit_bytes=50 * 1024 * 1024
        ),
    )(
        block_order, prompt_lengths, sink_logits[0],
        tokens, norm_gain, cosine, sine, w_key_value[0], w_query[0], w_out[0].T,
    )
    return hidden[None], cache[None]


def solution(mesh):
    in_specs = (
        P("groups", "seq", None),
        P("groups"),
        P("groups"),
        P("section", None),
        P("section", None, "seq"),
        P("section", None, None),
        P("section", "seq", None),
        P("section", None),
    )
    out_specs = (P("section", "groups", "seq", None), P("section", "groups", "seq", None))
    shape = tuple(mesh.shape[name] for name in ("groups", "section", "seq"))
    return jax.shard_map(
        functools.partial(per_device, shape),
        mesh=mesh, in_specs=in_specs, out_specs=out_specs, check_vma=False,
    )
```

```python
import functools
import math

import jax
import jax.numpy as jnp
from jax import lax
from jax.experimental import pallas as pl
from jax.experimental.pallas import tpu as pltpu
from jax.sharding import PartitionSpec as P

HEAD_DIM = 64
WIN = 128
LANES = 128


THETA = 150000.0
EPSILON = 1e-05
MESH = pl.DeviceIdType.MESH
F32 = jnp.float32
BF16 = jnp.bfloat16
QUERY_CUTS = 3
OUT_CUTS = 3
HOP_CUTS = 3


def rotary(positions, head_size):
    half = head_size // 2
    freq = jnp.exp(jnp.arange(half, dtype=F32) * (-2.0 * math.log(THETA) / head_size))
    angles = positions.astype(F32)[:, None] * freq[None, :]
    return jnp.cos(angles), jnp.sin(angles)


def kernel(
    shape,
    order_ref, length_ref, sink_ref,
    tokens_ref, gain_ref, cos_ref, sin_ref, pair_ref, query_hbm, out_hbm,
    hidden_ref, cache_ref,
    query_w, out_w, arrive, window, hbuf, normed_ref, qbuf, cbuf,
    local_sem, x_send, x_recv, y_send, y_recv, d_send, d_recv, own_send, own_recv,
    w_send, w_recv, z_send, z_recv,
):
    groups, sections, seq = shape
    chips = seq // 2
    g = lax.axis_index("groups")
    sec = lax.axis_index("section")
    q = lax.axis_index("seq")
    chip, core = q // 2, q % 2
    partner = chip * 2 + (1 - core)
    micro, rows, width = tokens_ref.shape
    shard = query_w.shape[2]
    heads_width = seq * shard
    kv_width = pair_ref.shape[1] // 2
    kv_heads = kv_width // HEAD_DIM
    group = heads_width // kv_width
    keep = min(WIN, rows)
    depth = WIN // keep

    mine = [
        pltpu.make_async_copy(query_hbm, query_w.at[q], local_sem.at[0]),
        pltpu.make_async_copy(
            out_hbm, out_w.at[:, pl.ds(pl.multiple_of(q * shard, shard), shard)], local_sem.at[1]
        ),
    ]
    for copy in mine:
        copy.start()

    barrier = pltpu.get_barrier_semaphore()
    greeted = 0
    for d in range(1, seq):
        pl.semaphore_signal(barrier, 1, device_id={"seq": (q + d) % seq}, device_id_type=MESH)
        greeted += 1
    for e in range(1, groups):
        pl.semaphore_signal(barrier, 1, device_id={"groups": (g + e) % groups}, device_id_type=MESH)
        greeted += 1
    for s in sorted({1 % sections, (sections - 1) % sections} - {0}):
        pl.semaphore_signal(barrier, 1, device_id={"section": (sec + s) % sections}, device_id_type=MESH)
        greeted += 1
    for off in range(1, depth + 1):

        @pl.when(q < off)
        def _():
            window[:, off - 1] = jnp.zeros((micro, keep, 2 * kv_width), BF16)

    pl.semaphore_wait(barrier, greeted)

    cuts = (QUERY_CUTS, OUT_CUTS)
    lengths = (width // groups // QUERY_CUTS, width // groups // OUT_CUTS)

    def piece(kind, owner, part, k):
        size = lengths[kind]
        first = (part * cuts[kind] + k) * size
        if kind == 0:
            return query_w.at[owner, pl.ds(pl.multiple_of(first, 16), size)]
        return out_w.at[
            pl.ds(pl.multiple_of(first, 16), size), pl.ds(pl.multiple_of(owner * shard, shard), shard)
        ]

    def whole(kind, owner):
        if kind == 0:
            return query_w.at[owner]
        return out_w.at[:, pl.ds(pl.multiple_of(owner * shard, shard), shard)]

    def remote(ref, send, recv, target):
        return pltpu.make_async_remote_copy(
            src_ref=ref, dst_ref=ref, send_sem=send, recv_sem=recv,
            device_id=target, device_id_type=MESH,
        )

    def x_copy(kind, d, k, owner):
        return remote(
            piece(kind, owner, g, k), x_send.at[kind, d, k], x_recv.at[kind, d, k],
            {"seq": ((chip + d) % chips) * 2 + core},
        )

    def y_copy(kind, d, k, e, owner, part):
        return remote(
            piece(kind, owner, part, k), y_send.at[kind, d, k, e], y_recv.at[kind, d, k, e],
            {"groups": (g + e) % groups},
        )

    def d_copy(kind, d, k, e, owner):
        return remote(
            piece(kind, owner, (g - e + groups) % groups, k), d_send.at[kind, d, k, e],
            d_recv.at[kind, d, k, e], {"seq": partner},
        )

    def own_copy(kind, owner):
        return remote(whole(kind, owner), own_send.at[kind], own_recv.at[kind], {"seq": partner})

    plan = [(kind, k, d) for kind in range(2) for k in range(cuts[kind]) for d in range(1, chips)]
    for kind in range(2):
        mine[kind].wait()
        for k in range(cuts[kind]):
            for d in range(1, chips):
                x_copy(kind, d, k, q).start()
        own_copy(kind, q).start()

    lane = lax.broadcasted_iota(jnp.int32, (rows, LANES), 1)
    first_half = (lane % HEAD_DIM) < (HEAD_DIM // 2)
    low = lane < HEAD_DIM
    cosine = cos_ref[...]
    sine = sin_ref[...]
    half = HEAD_DIM // 2

    def rotate(tile):
        swapped = jnp.where(
            first_half, pltpu.roll(tile, LANES - half, 1), pltpu.roll(tile, half, 1)
        )
        return tile * cosine + swapped * sine

    step = -(-width // (HOP_CUTS * LANES)) * LANES
    edges = [(c * step, min(step, width - c * step)) for c in range(HOP_CUTS)]

    def z_copy(t, c):
        columns = pl.ds(*edges[c])
        return pltpu.make_async_remote_copy(
            src_ref=hidden_ref.at[t, :, columns], dst_ref=arrive.at[t, :, columns],
            send_sem=z_send.at[t, c], recv_sem=z_recv.at[t, c], device_id={"section": (sec + 1) % sections}, device_id_type=MESH,
        )

    def w_copy(t, off, side):
        columns = pl.ds(side * kv_width, kv_width)
        return pltpu.make_async_remote_copy(
            src_ref=cache_ref.at[t, pl.ds(rows - keep, keep), columns],
            dst_ref=window.at[t, off - 1, :, columns],
            send_sem=w_send.at[t, off - 1, side], recv_sem=w_recv.at[t, off - 1, side],
            device_id={"seq": (q + off) % seq}, device_id_type=MESH,
        )

    def enter(t):
        block = order_ref[t]

        @pl.when(sec == 0)
        def _():
            hbuf[t] = tokens_ref[block]

        @pl.when(sec > 0)
        def _():
            for c in range(HOP_CUTS):
                z_copy(t, c).wait_recv()
            hbuf[t] = arrive[t]

        widened = hbuf[t].astype(F32)
        scale = lax.rsqrt(jnp.mean(widened * widened, -1, keepdims=True) + EPSILON)
        normed_ref[t] = (widened * scale * gain_ref[...]).astype(BF16)
        keys = jnp.dot(normed_ref[t], pair_ref[:, :kv_width], preferred_element_type=F32)
        for p in range(kv_width // LANES):
            tile = slice(p * LANES, (p + 1) * LANES)
            cache_ref[t, :, tile] = rotate(keys[:, tile]).astype(BF16)
        for off in range(1, depth + 1):

            @pl.when(q + off < seq)
            def _():
                w_copy(t, off, 0).start()

        values = jnp.dot(normed_ref[t], pair_ref[:, kv_width:], preferred_element_type=F32)
        cache_ref[t, :, kv_width:] = values.astype(BF16)
        for off in range(1, depth + 1):

            @pl.when(q + off < seq)
            def _():
                w_copy(t, off, 1).start()

    def attend(t, heads):
        length = length_ref[order_ref[t]]
        normed = normed_ref[t]

        def ask(s):
            queries = jnp.dot(normed, query_w[s], preferred_element_type=F32)
            for p in range(shard // LANES):
                rotated = rotate(queries[:, p * LANES:(p + 1) * LANES]) * 0.125
                qbuf[:, s * shard + p * LANES:s * shard + (p + 1) * LANES] = rotated.astype(BF16)

        per_head = seq // kv_heads
        for s in range(heads[0] * per_head, (heads[-1] + 1) * per_head):
            ask(s)

        if heads[0] == 0:
            for off in range(1, depth + 1):

                @pl.when(q >= off)
                def _():
                    w_copy(t, off, 0).wait_recv()
                    w_copy(t, off, 1).wait_recv()

        span = WIN + rows
        row = lax.broadcasted_iota(jnp.int32, (rows, span), 0)
        col = lax.broadcasted_iota(jnp.int32, (rows, span), 1) - WIN
        column = col + q * rows
        allowed = (col <= row) & (row - col < WIN) & (column >= 0)
        allowed = allowed & ((column < length) | (col == row))
        bias = jnp.where(allowed, F32(0.0), F32(-1e30))
        tiles = group // 2

        def span_of(first):
            at = slice(first, first + HEAD_DIM)
            parts = [window[t, off - 1, :, at] for off in range(depth, 0, -1)]
            return jnp.concatenate(parts + [cache_ref[t, :, at]], 0)

        def score(h):
            head = span_of(h * HEAD_DIM)
            stack = []
            for p in range(tiles):
                at = (h * tiles + p) * LANES
                pair = qbuf[:, at:at + LANES]
                zero = jnp.zeros_like(pair)
                stack += [jnp.where(low, pair, zero), jnp.where(low, zero, pair)]
            return lax.dot_general(
                jnp.concatenate(stack, 0), jnp.concatenate([head, head], 1),
                (((1,), (1,)), ((), ())), preferred_element_type=F32,
            )

        def mix(h, scores):
            head = span_of(kv_width + h * HEAD_DIM)
            values = jnp.concatenate([head, head, jnp.ones((span, LANES), BF16)], 1)
            expos, rest = [], []
            for j in range(group):
                sink = sink_ref[h * group + j]
                masked = scores[j * rows:(j + 1) * rows] + bias
                top = jnp.maximum(jnp.max(masked, -1, keepdims=True), sink)
                expos.append(jnp.exp(masked - top).astype(BF16))
                rest.append(jnp.exp(sink - top))
            summed = jnp.dot(jnp.concatenate(expos, 0), values, preferred_element_type=F32)
            for p in range(tiles):
                at = (h * tiles + p) * LANES
                sides = []
                for j in (2 * p, 2 * p + 1):
                    some = summed[j * rows:(j + 1) * rows]
                    sides.append((some[:, :LANES], some[:, LANES:] + rest[j]))
                context = jnp.where(low, sides[0][0], sides[1][0])
                context = context / jnp.where(low, sides[0][1], sides[1][1])
                cbuf[:, at:at + LANES] = context.astype(BF16)

        scores = score(heads[0])
        for h in heads:
            following = score(h + 1) if h + 1 in heads else None
            mix(h, scores)
            scores = following

    @pl.when(sec == 0)
    def _():
        @pl.loop(0, micro)
        def _(t):
            enter(t)

    def source(d, which):
        return ((chip - d + chips) % chips) * 2 + which

    def relay_y(kind, k, d):
        for e in range(1, groups):
            y_copy(kind, d, k, e, source(d, core), (g - e + groups) % groups).wait_recv()
            d_copy(kind, d, k, e, source(d, core)).start()

    previous = None
    for kind, k, d in plan:
        x_copy(kind, d, k, source(d, core)).wait_recv()
        for e in range(1, groups):
            y_copy(kind, d, k, e, source(d, core), g).start()
        d_copy(kind, d, k, 0, source(d, core)).start()
        if previous is not None:
            relay_y(*previous)
        previous = (kind, k, d)
        if kind == 1 and d == 1 and k == 1:
            own_copy(0, partner).wait_recv()
            for one in plan:
                if one[0] == 0:
                    for e in range(groups):
                        d_copy(*one[:1], one[2], one[1], e, source(one[2], 1 - core)).wait_recv()
        if kind == 1 and d == 1 and k >= 1:
            share = kv_heads // 2

            @pl.when(sec == 0)
            def _():
                attend(0, tuple(range((k - 1) * share, k * share)))

    if previous is not None:
        relay_y(*previous)
    own_copy(1, partner).wait_recv()
    for kind, k, d in plan:
        for e in range(groups if kind else 0):
            d_copy(kind, d, k, e, source(d, 1 - core)).wait_recv()

    def slot(t, carry):
        @pl.when(sec > 0)
        def _():
            enter(t)

        @pl.when((sec > 0) | (t > 0))
        def _():
            attend(t, tuple(range(kv_heads)))

        for c, (first, size) in enumerate(edges):
            output = lax.dot_general(
                cbuf[...], out_w[first:first + size], (((1,), (1,)), ((), ())),
                preferred_element_type=F32,
            )
            columns = slice(first, first + size)
            hidden_ref[t, :, columns] = (hbuf[t, :, columns].astype(F32) + output).astype(BF16)

            @pl.when(sec + 1 < sections)
            def _():
                z_copy(t, c).start()

        return carry

    lax.fori_loop(0, micro, slot, 0)

    for kind, k, d in plan:
        x_copy(kind, d, k, q).wait_send()
        for e in range(1, groups):
            y_copy(kind, d, k, e, source(d, core), g).wait_send()
        for e in range(groups):
            d_copy(kind, d, k, e, source(d, core)).wait_send()
    for kind in range(2):
        own_copy(kind, q).wait_send()
    for t in range(micro):
        for off in range(1, depth + 1):

            @pl.when(q + off < seq)
            def _():
                w_copy(t, off, 0).wait_send()
                w_copy(t, off, 1).wait_send()

        @pl.when(sec + 1 < sections)
        def _():
            for c in range(HOP_CUTS):
                z_copy(t, c).wait_send()


def per_device(
    shape,
    tokens, block_order, prompt_lengths, norm_gain, w_query, w_key_value, w_out, sink_logits
):
    groups, sections, seq = shape
    micro, rows, width = tokens.shape
    shard = w_query.shape[2]
    pair_width = w_key_value.shape[2]
    chips = seq // 2
    keep = min(WIN, rows)
    depth = WIN // keep
    positions = lax.axis_index("seq") * rows + jnp.arange(rows, dtype=jnp.int32)
    cosine, sine = rotary(positions, HEAD_DIM)
    repeat = LANES // HEAD_DIM
    cosine = jnp.tile(jnp.concatenate([cosine, cosine], 1), (1, repeat))
    sine = jnp.tile(jnp.concatenate([-sine, sine], 1), (1, repeat))
    most = max(QUERY_CUTS, OUT_CUTS)
    dma = pltpu.SemaphoreType.DMA
    vmem = pl.BlockSpec(memory_space=pltpu.VMEM)
    smem = pl.BlockSpec(memory_space=pltpu.SMEM)
    hbm = pl.BlockSpec(memory_space=pl.ANY)
    hidden, cache = pl.pallas_call(
        functools.partial(kernel, shape),
        out_shape=(
            jax.ShapeDtypeStruct((micro, rows, width), BF16),
            jax.ShapeDtypeStruct((micro, rows, pair_width), BF16),
        ),
        in_specs=[smem] * 3 + [vmem] * 5 + [hbm] * 2,
        out_specs=(vmem, vmem),
        scratch_shapes=[
            pltpu.VMEM((seq, width, shard), BF16),
            pltpu.VMEM((width, seq * shard), BF16),
            pltpu.VMEM((micro, rows, width), BF16),
            pltpu.VMEM((micro, depth, keep, pair_width), BF16),
            pltpu.VMEM((micro, rows, width), BF16),
            pltpu.VMEM((micro, rows, width), BF16),
            pltpu.VMEM((rows, seq * shard), BF16),
            pltpu.VMEM((rows, seq * shard), BF16),
            dma((2,)),
            dma((2, chips, most)),
            dma((2, chips, most)),
            dma((2, chips, most, groups)),
            dma((2, chips, most, groups)),
            dma((2, chips, most, groups)),
            dma((2, chips, most, groups)),
            dma((2,)),
            dma((2,)),
            dma((micro, depth, 2)),
            dma((micro, depth, 2)),
            dma((micro, HOP_CUTS)),
            dma((micro, HOP_CUTS)),
        ],
        compiler_params=pltpu.CompilerParams(
            collective_id=0, has_side_effects=True, vmem_limit_bytes=50 * 1024 * 1024
        ),
    )(
        block_order, prompt_lengths, sink_logits[0],
        tokens, norm_gain, cosine, sine, w_key_value[0], w_query[0], w_out[0].T,
    )
    return hidden[None], cache[None]


def solution(mesh):
    in_specs = (
        P("groups", "seq", None),
        P("groups"),
        P("groups"),
        P("section", None),
        P("section", None, "seq"),
        P("section", None, None),
        P("section", "seq", None),
        P("section", None),
    )
    out_specs = (P("section", "groups", "seq", None), P("section", "groups", "seq", None))
    shape = tuple(mesh.shape[name] for name in ("groups", "section", "seq"))
    return jax.shard_map(
        functools.partial(per_device, shape),
        mesh=mesh, in_specs=in_specs, out_specs=out_specs, check_vma=False,
    )
```
